32 devices in a mesh: dp: 2 (over x), tp: 4 (over z), pp: 4 (over y, core).
Axes of the slice: x: 2, y: 2, z: 4, core: 2. Of those that a mesh axis runs over, the one named last changes fastest.
Arguments:
- x_in: bfloat16 [8, 2, 512, 768], P('dp'), parts along dimension 0
- seq_len: int32 [8, 2], P('dp'), parts along dimension 0
- dy_out: bfloat16 [8, 2, 512, 768], P('dp'), parts along dimension 0
- ln1_gain: float32 [4, 768], P('pp')
- ln1_bias: float32 [4, 768], P('pp')
- w_qkv: bfloat16 [4, 3, 768, 12, 64], P('pp', None, None, 'tp')
- b_qkv: float32 [4, 3, 12, 64], P('pp', None, 'tp')
- w_attn: bfloat16 [4, 12, 64, 768], P('pp', 'tp')
- b_attn: float32 [4, 768], P('pp')
- ln2_gain: float32 [4, 768], P('pp')
- ln2_bias: float32 [4, 768], P('pp')
- w_up: bfloat16 [4, 768, 3072], P('pp', None, 'tp')
- b_up: float32 [4, 3072], P('pp', 'tp')
- w_down: bfloat16 [4, 3072, 768], P('pp', 'tp')
- b_down: float32 [4, 768], P('pp')
Outputs:
- output 1: bfloat16 [4, 8, 2, 512, 768], P('pp', 'dp'), parts along dimension 1
- output 2: bfloat16 [4, 8, 2, 512, 768], P('pp', 'dp'), parts along dimension 1
- output 3: float32 [8, 768], P(('dp', 'pp')), parts along dimension 0
- output 4: float32 [8, 768], P(('dp', 'pp')), parts along dimension 0
- output 5: float32 [8, 3, 768, 12, 64], P(('dp', 'pp'), None, None, 'tp'), parts along dimension 0
- output 6: float32 [8, 3, 12, 64], P(('dp', 'pp'), None, 'tp'), parts along dimension 0
- output 7: float32 [8, 12, 64, 768], P(('dp', 'pp'), 'tp'), parts along dimension 0
- output 8: float32 [8, 768], P(('dp', 'pp')), parts along dimension 0
- output 9: float32 [8, 768], P(('dp', 'pp')), parts along dimension 0
- output 10: float32 [8, 768], P(('dp', 'pp')), parts along dimension 0
- output 11: float32 [8, 768, 3072], P(('dp', 'pp'), None, 'tp'), parts along dimension 0
- output 12: float32 [8, 3072], P(('dp', 'pp'), 'tp'), parts along dimension 0
- output 13: float32 [8, 3072, 768], P(('dp', 'pp'), 'tp'), parts along dimension 0
- output 14: float32 [8, 768], P(('dp', 'pp')), parts along dimension 0
There are 2 independent parts. The reference program is written for one: setup_inputs(seed, part) draws one part's arguments, and reference() takes and returns one part's arrays. A program takes and returns all parts, laid end to end along the dimension named above; an argument that names none is the same for every part.
All inputs are finite; a program needn't handle non-finite values.
Results may differ from the reference program's by a relative error of at most 0.02.
Values are sent between devices in bfloat16 or wider.
A program may use at most 1 GiB of HBM per device.

```python
import jax
import jax.numpy as jnp
from jax import lax

D = 768
HEADS = 12
HEAD = 64
FF = 3072
SEQ_LEN = 512
NUM_MICRO = 4
MICRO_ROWS = 2
STAGES = 4
LN_EPS = 1e-5
MASK_VALUE = -1e9


def setup_inputs(seed: int = 0, part: int = 0) -> dict:
    root_key = jax.random.key(seed)
    part_keys = jax.random.split(jax.random.fold_in(root_key, part), 3)
    shared_keys = jax.random.split(root_key, 12)
    micro_shape = (NUM_MICRO, MICRO_ROWS, SEQ_LEN, D)

    def draw_normal(rng_key, shape, factor):
        return jax.random.normal(rng_key, shape, jnp.float32) * factor

    lengths = jax.random.randint(part_keys[1], (NUM_MICRO, MICRO_ROWS), SEQ_LEN // 4, SEQ_LEN + 1, dtype=jnp.int32)
    dy_scale = (NUM_MICRO * MICRO_ROWS * SEQ_LEN) ** -0.25
    return {
        'x_in': draw_normal(part_keys[0], micro_shape, 1.0).astype(jnp.bfloat16),
        'seq_len': lengths.at[0, 0].set(SEQ_LEN),
        'dy_out': draw_normal(part_keys[2], micro_shape, dy_scale).astype(jnp.bfloat16),
        'ln1_gain': 1.0 + draw_normal(shared_keys[0], (STAGES, D), 0.2),
        'ln1_bias': draw_normal(shared_keys[1], (STAGES, D), 0.2),
        'w_qkv': draw_normal(shared_keys[2], (STAGES, 3, D, HEADS, HEAD), D ** -0.5).astype(jnp.bfloat16),
        'b_qkv': draw_normal(shared_keys[3], (STAGES, 3, HEADS, HEAD), 0.5),
        'w_attn': draw_normal(shared_keys[4], (STAGES, HEADS, HEAD, D), (HEADS * HEAD) ** -0.5).astype(jnp.bfloat16),
        'b_attn': draw_normal(shared_keys[5], (STAGES, D), 0.2),
        'ln2_gain': 1.0 + draw_normal(shared_keys[6], (STAGES, D), 0.2),
        'ln2_bias': draw_normal(shared_keys[7], (STAGES, D), 0.2),
        'w_up': draw_normal(shared_keys[8], (STAGES, D, FF), D ** -0.5).astype(jnp.bfloat16),
        'b_up': draw_normal(shared_keys[9], (STAGES, FF), 0.5),
        'w_down': draw_normal(shared_keys[10], (STAGES, FF, D), FF ** -0.5).astype(jnp.bfloat16),
        'b_down': draw_normal(shared_keys[11], (STAGES, D), 0.2),
    }


def layer_norm(h_f32, ln_gain, ln_bias):
    row_mean = jnp.mean(h_f32, axis=-1, keepdims=True)
    centred = h_f32 - row_mean
    row_var = jnp.mean(centred * centred, axis=-1, keepdims=True)
    return centred * lax.rsqrt(row_var + LN_EPS) * ln_gain + ln_bias


def to_bf16(value):
    return value.astype(jnp.bfloat16).astype(jnp.float32)


def layer_forward(h_in, key_ok, params):
    (ln1_gain, ln1_bias, w_qkv, b_qkv, w_attn, b_attn, ln2_gain, ln2_bias, w_up, b_up, w_down, b_down) = params
    x_f32 = h_in.astype(jnp.float32)
    normed = to_bf16(layer_norm(x_f32, ln1_gain, ln1_bias))
    qkv_all = to_bf16(jnp.einsum('bsd,tdhk->tbshk', normed, w_qkv) + b_qkv[:, None, None])
    scores = jnp.einsum('bqhk,bshk->bhqs', qkv_all[0], qkv_all[1]) * (HEAD ** -0.5)
    scores = jnp.where(key_ok[:, None, None, :], scores, MASK_VALUE)
    probs = to_bf16(jax.nn.softmax(scores, axis=-1))
    context = to_bf16(jnp.einsum('bhqs,bshk->bqhk', probs, qkv_all[2]))
    mid_act = (x_f32 + jnp.einsum('bqhk,hkd->bqd', context, w_attn) + b_attn).astype(jnp.bfloat16)
    mid_f32 = mid_act.astype(jnp.float32)
    normed2 = to_bf16(layer_norm(mid_f32, ln2_gain, ln2_bias))
    hidden = to_bf16(jax.nn.gelu(jnp.einsum('bsd,df->bsf', normed2, w_up) + b_up, approximate=False))
    return (mid_f32 + jnp.einsum('bsf,fd->bsd', hidden, w_down) + b_down).astype(jnp.bfloat16)


def reference(x_in, seq_len, dy_out, ln1_gain, ln1_bias, w_qkv, b_qkv, w_attn, b_attn, ln2_gain, ln2_bias, w_up, b_up, w_down, b_down):
    params = tuple(weight.astype(jnp.float32) for weight in (ln1_gain, ln1_bias, w_qkv, b_qkv, w_attn, b_attn, ln2_gain, ln2_bias, w_up, b_up, w_down, b_down))
    key_ok = jnp.arange(SEQ_LEN)[None, None, :] < seq_len[:, :, None]

    def micro_step(grad_sum, micro_in):
        x_micro, ok_micro, dy_micro = micro_in

        def fwd_layer(h_cur, layer_params):
            h_next = layer_forward(h_cur, ok_micro, layer_params)
            return h_next, (h_cur, h_next)

        _, (layer_ins, layer_outs) = lax.scan(fwd_layer, x_micro, params)

        def bwd_layer(g_cur, packed):
            h_cur, layer_params = packed
            _, back_fn = jax.vjp(lambda h_arg, p_arg: layer_forward(h_arg, ok_micro, p_arg), h_cur, layer_params)
            g_prev, g_params = back_fn(g_cur)
            return g_prev, (g_prev, g_params)

        _, (layer_dx, layer_grads) = lax.scan(bwd_layer, dy_micro, (layer_ins, params), reverse=True)
        grad_sum = jax.tree.map(jnp.add, grad_sum, layer_grads)
        return grad_sum, (layer_outs, layer_dx)

    grad_init = jax.tree.map(jnp.zeros_like, params)
    grads, (outs_all, dx_all) = lax.scan(micro_step, grad_init, (x_in, key_ok, dy_out))
    stage_out = jnp.swapaxes(outs_all, 0, 1)
    stage_dx = jnp.swapaxes(dx_all, 0, 1)
    return (stage_out, stage_dx, grads[0], grads[1], grads[2], grads[3], grads[4], grads[5], grads[6], grads[7], grads[8], grads[9], grads[10], grads[11])
```

```python
import functools

import jax
import jax.numpy as jnp
from jax import lax
from jax.experimental import pallas as pl
from jax.experimental.pallas import tpu as pltpu
from jax.sharding import Mesh, PartitionSpec as P

LN_EPS = 1e-5
MASK_VALUE = -1e9
F32 = jnp.float32
BF16 = jnp.bfloat16
NT = (((1,), (1,)), ((), ()))
NN = (((1,), (0,)), ((), ()))
TN = (((0,), (0,)), ((), ()))


def dot(lhs, rhs, dims):
    return lax.dot_general(lhs, rhs, dims, preferred_element_type=F32)


def attn_fwd_kernel(len_ref, q_ref, k_ref, v_ref, ctx_ref):
    rows = q_ref.shape[0]
    key_ok = lax.broadcasted_iota(jnp.int32, (rows, rows), 1) < len_ref[0]
    parts = []
    for half in range(2):
        cols = slice(half * 64, half * 64 + 64)
        scores = dot(q_ref[:, cols], k_ref[:, cols], NT) * 0.125
        scores = jnp.where(key_ok, scores, MASK_VALUE)
        expd = jnp.exp(scores - jnp.max(scores, axis=-1, keepdims=True))
        prob = (expd * (1.0 / jnp.sum(expd, axis=-1, keepdims=True))).astype(BF16)
        parts.append(dot(prob, v_ref[:, cols], NN).astype(BF16))
    ctx_ref[...] = jnp.concatenate(parts, axis=1)


def attn_bwd_kernel(len_ref, q_ref, k_ref, v_ref, dctx_ref, dqkv_ref):
    rows = q_ref.shape[0]
    width = dqkv_ref.shape[1] // 3
    key_ok = lax.broadcasted_iota(jnp.int32, (rows, rows), 0) < len_ref[0]
    pieces = ([], [], [])
    for half in range(2):
        cols = slice(half * 64, half * 64 + 64)
        q, k, v, dctx = q_ref[:, cols], k_ref[:, cols], v_ref[:, cols], dctx_ref[:, cols]
        scores = dot(k, q, NT) * 0.125
        scores = jnp.where(key_ok, scores, MASK_VALUE)
        expd = jnp.exp(scores - jnp.max(scores, axis=0, keepdims=True))
        prob = expd * (1.0 / jnp.sum(expd, axis=0, keepdims=True))
        d_prob = dot(v, dctx, NT)
        delta = jnp.sum(d_prob * prob, axis=0, keepdims=True)
        d_scores = (prob * (d_prob - delta) * 0.125).astype(BF16)
        pieces[0].append(dot(d_scores, k, TN).astype(BF16))
        pieces[1].append(dot(d_scores, q, NN).astype(BF16))
        pieces[2].append(dot(prob.astype(BF16), dctx, NN).astype(BF16))
    pair = pl.program_id(0)
    for part in range(3):
        start = pl.multiple_of(part * width + pair * 128, 128)
        dqkv_ref[:, pl.ds(start, 128)] = jnp.concatenate(pieces[part], axis=1)


def col_spec(rows, offset):
    return pl.BlockSpec((rows, 128), lambda i: (0, offset + i))


SMEM_SPEC = pl.BlockSpec(memory_space=pltpu.SMEM)


def attn_fwd(qkv, length):
    rows, width = qkv.shape[0], qkv.shape[1] // 3
    pairs = width // 128
    return pl.pallas_call(
        attn_fwd_kernel,
        grid=(pairs,),
        out_shape=jax.ShapeDtypeStruct((rows, width), BF16),
        in_specs=[SMEM_SPEC] + [col_spec(rows, part * pairs) for part in range(3)],
        out_specs=col_spec(rows, 0),
        cost_estimate=pl.CostEstimate(flops=8 * pairs * rows * rows * 64 * 4, bytes_accessed=8 * rows * width, transcendentals=2 * pairs * rows * rows),
        name='attn_fwd',
    )(length, qkv, qkv, qkv)


def attn_bwd(qkv, dctx, length):
    rows, width = qkv.shape[0], qkv.shape[1] // 3
    pairs = width // 128
    return pl.pallas_call(
        attn_bwd_kernel,
        grid=(pairs,),
        out_shape=jax.ShapeDtypeStruct((rows, 3 * width), BF16),
        in_specs=[SMEM_SPEC] + [col_spec(rows, part * pairs) for part in range(3)] + [col_spec(rows, 0)],
        out_specs=pl.BlockSpec((rows, 3 * width), lambda i: (0, 0)),
        cost_estimate=pl.CostEstimate(flops=20 * pairs * rows * rows * 64 * 4, bytes_accessed=14 * rows * width, transcendentals=2 * pairs * rows * rows),
        name='attn_bwd',
    )(length, qkv, qkv, qkv, dctx)


def normalise(v_bf):
    v = v_bf.astype(F32)
    centred = v - jnp.mean(v, axis=-1, keepdims=True)
    rstd = lax.rsqrt(jnp.mean(centred * centred, axis=-1, keepdims=True) + LN_EPS)
    return centred * rstd, rstd


def layer_norm(v_bf, gain, bias):
    return (normalise(v_bf)[0] * gain + bias).astype(BF16)


def norm_back(v_bf, gain, d_out_bf, residual_bf):
    xhat, rstd = normalise(v_bf)
    d_out = d_out_bf.astype(F32)
    d_hat = d_out * gain
    d_in = rstd * (d_hat - jnp.mean(d_hat, axis=-1, keepdims=True) - xhat * jnp.mean(d_hat * xhat, axis=-1, keepdims=True))
    d_v = (residual_bf.astype(F32) + d_in).astype(BF16)
    return d_v, jnp.sum(d_out * xhat, axis=0), jnp.sum(d_out, axis=0)


def gelu(value):
    return jax.nn.gelu(value, approximate=False)


def gelu_back(up, d_hidden_bf):
    return jax.vjp(gelu, up)[1](d_hidden_bf.astype(F32))[0]


def layer_forward(h_in, params, length):
    w_att, w_up, w_down, vec, b_qkv, b_up = params
    n_qkv = b_qkv.shape[0]
    normed = layer_norm(h_in, vec[0], vec[1])
    qkv = (dot(normed, w_att[:n_qkv], NT) + b_qkv).astype(BF16)
    context = attn_fwd(qkv, length)
    mid = (h_in.astype(F32) + dot(context, w_att[n_qkv:], NN) + vec[2]).astype(BF16)
    normed2 = layer_norm(mid, vec[3], vec[4])
    up = dot(normed2, w_up, NT) + b_up
    hidden = gelu(up).astype(BF16)
    out = (mid.astype(F32) + dot(hidden, w_down, NN) + vec[5]).astype(BF16)
    return out, (h_in, normed, qkv, context, mid, up)


def layer_backward(g_out, saved, params, length):
    w_att, w_up, w_down, vec, b_qkv, b_up = params
    n_qkv = b_qkv.shape[0]
    h_in, normed, qkv, context, mid, up = saved
    d_hidden = dot(g_out, w_down, NT).astype(BF16)
    d_up = gelu_back(up, d_hidden).astype(BF16)
    d_normed2 = dot(d_up, w_up, NN).astype(BF16)
    d_mid, d_gain2, d_bias2 = norm_back(mid, vec[3], d_normed2, g_out)
    d_context = dot(d_mid, w_att[n_qkv:], NT).astype(BF16)
    d_qkv = attn_bwd(qkv, d_context, length)
    d_normed = dot(d_qkv, w_att[:n_qkv], NN).astype(BF16)
    d_x, d_gain1, d_bias1 = norm_back(h_in, vec[0], d_normed, d_mid)
    d_b_attn = jnp.sum(d_mid, axis=0, dtype=F32)
    d_b_qkv = jnp.sum(d_qkv, axis=0, dtype=F32).reshape(3, -1)
    small = jnp.concatenate([jnp.stack([d_gain1, d_bias1, d_b_attn, d_gain2, d_bias2]), d_b_qkv])
    return d_x, (d_qkv, d_mid, context, normed, small)


def solution(mesh):
    n_dp, n_tp, n_pp = mesh.shape['dp'], mesh.shape['tp'], mesh.shape['pp']
    split = Mesh(mesh.devices.reshape(n_dp, n_tp, n_pp // 2, 2), ('dp', 'tp', 'py', 'core'))
    pp = ('py', 'core')
    act_spec = P('dp', None, None, None)
    param_specs = (P(pp, None), P(pp, None), P(pp, None, None, 'tp', None), P(pp, None, 'tp', None), P(pp, 'tp', None, None), P(pp, None), P(pp, None), P(pp, None), P(pp, None, 'tp'), P(pp, 'tp'), P(pp, 'tp', None), P(pp, None))
    gp = ('dp', 'py', 'core')
    grad_specs = (P(gp, None), P(gp, None), P(gp, None, None, 'tp', None), P(gp, None, 'tp', None), P(gp, 'tp', None, None), P(gp, None), P(gp, None), P(gp, None), P(gp, None, 'tp'), P(gp, 'tp'), P(gp, 'tp', None), P(gp, None))
    stage_spec = P(pp, 'dp', None, None, None)
    swap = [(0, 1), (1, 0)]

    def body(x_in, seq_len, dy_out, *weights):
        (ln1_gain, ln1_bias, w_qkv, b_qkv, w_attn, b_attn, ln2_gain, ln2_bias, w_up, b_up, w_down, b_down) = tuple(weight[0] for weight in weights)
        dp_id, tp_id, py_id, core_id = (lax.axis_index(name) for name in ('dp', 'tp', 'py', 'core'))
        n_micro, _, rows, width = x_in.shape
        n_local = w_attn.shape[0] * w_attn.shape[1]
        first_core, first_pair = core_id == 0, py_id == 0

        def gather_weight(shard):
            half = shard.shape[0] // n_dp
            piece = lax.dynamic_slice_in_dim(shard, dp_id * half, half, 0)
            return lax.all_gather(piece, ('tp', 'dp'), axis=0, tiled=True)

        att_shard = jnp.concatenate([w_qkv.reshape(3, width, n_local).transpose(0, 2, 1).reshape(3 * n_local, width), w_attn.reshape(n_local, width)])
        att_full = gather_weight(att_shard).reshape(n_tp, 4, n_local, width).transpose(1, 0, 2, 3).reshape(4 * n_tp * n_local, width)
        up_full = gather_weight(w_up.T)
        down_full = gather_weight(w_down)
        both = [lax.all_gather(full, 'core', axis=0) for full in (att_full, up_full, down_full)]

        b_qkv_flat = b_qkv.reshape(3 * n_local)
        packed = jnp.concatenate([jnp.stack([ln1_gain, ln1_bias, b_attn, ln2_gain, ln2_bias, b_down]), jnp.pad(b_qkv_flat, (0, width - 3 * n_local))[None], b_up.reshape(-1, width)])
        packed = lax.all_gather(packed, ('core', 'tp'), axis=0).reshape(2, n_tp, -1, width)

        def layer_params(layer):
            b_qkv_full = packed[layer, :, 6, :3 * n_local].reshape(n_tp, 3, n_local).transpose(1, 0, 2).reshape(-1)
            b_up_full = packed[layer, :, 7:].reshape(-1)
            return tuple(arr[layer] for arr in both) + (packed[layer, 0, :6], b_qkv_full, b_up_full)

        params = (layer_params(0), layer_params(1))

        def my_sequence(array):
            return lax.dynamic_slice(array, (tp_id, core_id, 0, 0), (1, 1, rows, width)).reshape(rows, width)

        length = lax.dynamic_slice(seq_len, (tp_id, core_id), (1, 1)).reshape(1)

        def forward(h):
            mid, saved0 = layer_forward(h, params[0], length)
            out, saved1 = layer_forward(mid, params[1], length)
            return (mid, out), (saved0, saved1)

        def backward(g, saved):
            dx1, keep1 = layer_backward(g, saved[1], params[1], length)
            dx0, keep0 = layer_backward(dx1, saved[0], params[0], length)
            return (dx0, dx1), (keep0, keep1)

        outs_a, saved_a = forward(my_sequence(x_in))
        outs_b, saved_b = forward(lax.ppermute(outs_a[1], 'py', [(0, 1)]))

        def own_stage(phase0, phase1):
            by_layer = [jnp.where(first_pair, phase0[layer], phase1[layer]) for layer in range(2)]
            keep = jnp.where(first_core, by_layer[0], by_layer[1])
            other = lax.ppermute(jnp.where(first_core, by_layer[1], by_layer[0]), 'core', swap)
            return jnp.stack([jnp.where(first_core, keep, other), jnp.where(first_core, other, keep)])

        def gather_tokens(phase0, phase1):
            return lax.all_gather(own_stage(phase0, phase1), 'tp', axis=0)

        stage_out = gather_tokens(outs_a, outs_b)
        mid_all = gather_tokens([saved[4] for saved in saved_a], [saved[4] for saved in saved_b])

        dxs_b, keeps_b = backward(my_sequence(dy_out), saved_b)
        dxs_a, keeps_a = backward(lax.ppermute(dxs_b[0], 'py', [(1, 0)]), saved_a)

        stage_dx = gather_tokens(dxs_a, dxs_b)
        next_dx = lax.ppermute(stage_dx, pp, [(s + 1, s) for s in range(n_pp - 1)])
        is_last = (~first_pair) & (~first_core)
        g_all = jnp.where(is_last, dy_out, next_dx).reshape(-1, width)

        d_qkv, d_mid, context, normed, small = (own_stage([keep[i] for keep in keeps_a], [keep[i] for keep in keeps_b]) for i in range(5))
        tokens = 2 * rows
        gw_qkv = dot(d_qkv.reshape(tokens, -1), normed.reshape(tokens, -1), TN)
        gw_attn = dot(context.reshape(tokens, -1), d_mid.reshape(tokens, -1), TN)
        small = small[0] + small[1]
        gw_att = jnp.concatenate([gw_qkv, gw_attn]).reshape(4, n_tp, n_local, width).transpose(1, 0, 2, 3).reshape(n_tp, 4 * n_local, width)
        gb_qkv = small[5:].reshape(3, n_tp, n_local).transpose(1, 0, 2).reshape(n_tp, 1, 3 * n_local)
        gb_qkv = jnp.pad(gb_qkv, ((0, 0), (0, 2), (0, width - 3 * n_local)))
        payload = jnp.concatenate([gw_att, jnp.broadcast_to(small[None, :5], (n_tp, 5, width)), gb_qkv], axis=1)
        reduced = lax.psum_scatter(payload, 'tp', scatter_dimension=0, tiled=False)
        g_qkv = reduced[:3 * n_local].reshape(3, n_local, width).transpose(0, 2, 1).reshape(w_qkv.shape)
        g_attn = reduced[3 * n_local:4 * n_local].reshape(w_attn.shape)
        g_vec = reduced[4 * n_local:]

        mid_flat = mid_all.reshape(-1, width)
        normed2 = layer_norm(mid_flat, ln2_gain, ln2_bias)
        up = dot(normed2, w_up, NN) + b_up
        hidden = gelu(up).astype(BF16)
        d_hidden = dot(g_all, w_down, NT).astype(BF16)
        d_up = gelu_back(up, d_hidden)
        g_w_up = dot(normed2, d_up.astype(BF16), TN)
        g_w_down = dot(hidden, g_all, TN)
        g_b_up = jnp.sum(d_up, axis=0)
        g_b_down = jnp.sum(g_all, axis=0, dtype=F32)

        grads = (g_vec[0], g_vec[1], g_qkv, g_vec[5, :3 * n_local].reshape(b_qkv.shape), g_attn, g_vec[2], g_vec[3], g_vec[4], g_w_up, g_b_up, g_w_down, g_b_down)
        return (stage_out[None], stage_dx[None]) + tuple(grad[None] for grad in grads)

    return jax.shard_map(body, mesh=split, in_specs=(act_spec, P('dp', None), act_spec) + param_specs, out_specs=(stage_spec, stage_spec) + grad_specs, check_vma=False)
```

```python
import jax
import jax.numpy as jnp
from jax import lax
from jax.experimental import pallas as pl
from jax.experimental.pallas import tpu as pltpu
from jax.experimental.layout import Layout, with_layout_constraint
from jax.sharding import Mesh, PartitionSpec as P

LN_EPS = 1e-5
MASK_VALUE = -1e9
ROW_MAJOR = Layout((0, 1))
F32 = jnp.float32
BF16 = jnp.bfloat16
NT = (((1,), (1,)), ((), ()))
NN = (((1,), (0,)), ((), ()))
TN = (((0,), (0,)), ((), ()))


def dot(lhs, rhs, dims):
    return lax.dot_general(lhs, rhs, dims, preferred_element_type=F32)


def attn_fwd_kernel(len_ref, q_ref, k_ref, v_ref, ctx_ref):
    rows = q_ref.shape[0]
    key_ok = lax.broadcasted_iota(jnp.int32, (rows, rows), 1) < len_ref[0]
    parts = []
    for half in range(2):
        cols = slice(half * 64, half * 64 + 64)
        scores = dot(q_ref[:, cols], k_ref[:, cols], NT) * 0.125
        scores = jnp.where(key_ok, scores, MASK_VALUE)
        expd = jnp.exp(scores - jnp.max(scores, axis=-1, keepdims=True))
        prob = (expd * (1.0 / jnp.sum(expd, axis=-1, keepdims=True))).astype(BF16)
        parts.append(dot(prob, v_ref[:, cols], NN).astype(BF16))
    ctx_ref[...] = jnp.concatenate(parts, axis=1)


def attn_bwd_kernel(len_ref, q_ref, k_ref, v_ref, dctx_ref, dqkv_ref):
    rows = q_ref.shape[0]
    width = dqkv_ref.shape[1] // 3
    key_ok = lax.broadcasted_iota(jnp.int32, (rows, rows), 0) < len_ref[0]
    pieces = ([], [], [])
    for half in range(2):
        cols = slice(half * 64, half * 64 + 64)
        q, k, v, dctx = q_ref[:, cols], k_ref[:, cols], v_ref[:, cols], dctx_ref[:, cols]
        scores = dot(k, q, NT) * 0.125
        scores = jnp.where(key_ok, scores, MASK_VALUE)
        expd = jnp.exp(scores - jnp.max(scores, axis=0, keepdims=True))
        prob = expd * (1.0 / jnp.sum(expd, axis=0, keepdims=True))
        d_prob = dot(v, dctx, NT)
        delta = jnp.sum(d_prob * prob, axis=0, keepdims=True)
        d_scores = (prob * (d_prob - delta) * 0.125).astype(BF16)
        pieces[0].append(dot(d_scores, k, TN).astype(BF16))
        pieces[1].append(dot(d_scores, q, NN).astype(BF16))
        pieces[2].append(dot(prob.astype(BF16), dctx, NN).astype(BF16))
    pair = pl.program_id(0)
    for part in range(3):
        start = pl.multiple_of(part * width + pair * 128, 128)
        dqkv_ref[:, pl.ds(start, 128)] = jnp.concatenate(pieces[part], axis=1)


def col_spec(rows, offset):
    return pl.BlockSpec((rows, 128), lambda i: (0, offset + i))


SMEM_SPEC = pl.BlockSpec(memory_space=pltpu.SMEM)


def attn_fwd(qkv, length):
    rows, width = qkv.shape[0], qkv.shape[1] // 3
    pairs = width // 128
    return pl.pallas_call(
        attn_fwd_kernel,
        grid=(pairs,),
        out_shape=jax.ShapeDtypeStruct((rows, width), BF16),
        in_specs=[SMEM_SPEC] + [col_spec(rows, part * pairs) for part in range(3)],
        out_specs=col_spec(rows, 0),
        cost_estimate=pl.CostEstimate(flops=8 * pairs * rows * rows * 64 * 4, bytes_accessed=8 * rows * width, transcendentals=2 * pairs * rows * rows),
        name='attn_fwd',
    )(length, qkv, qkv, qkv)


def attn_bwd(qkv, dctx, length):
    rows, width = qkv.shape[0], qkv.shape[1] // 3
    pairs = width // 128
    return pl.pallas_call(
        attn_bwd_kernel,
        grid=(pairs,),
        out_shape=jax.ShapeDtypeStruct((rows, 3 * width), BF16),
        in_specs=[SMEM_SPEC] + [col_spec(rows, part * pairs) for part in range(3)] + [col_spec(rows, 0)],
        out_specs=pl.BlockSpec((rows, 3 * width), lambda i: (0, 0)),
        cost_estimate=pl.CostEstimate(flops=20 * pairs * rows * rows * 64 * 4, bytes_accessed=14 * rows * width, transcendentals=2 * pairs * rows * rows),
        name='attn_bwd',
    )(length, qkv, qkv, qkv, dctx)


def normalise(v_bf):
    v = v_bf.astype(F32)
    centred = v - jnp.mean(v, axis=-1, keepdims=True)
    rstd = lax.rsqrt(jnp.mean(centred * centred, axis=-1, keepdims=True) + LN_EPS)
    return centred * rstd, rstd


def layer_norm(v_bf, gain, bias):
    return (normalise(v_bf)[0] * gain + bias).astype(BF16)


def norm_back(v_bf, gain, d_out_bf, residual_bf):
    xhat, rstd = normalise(v_bf)
    d_out = d_out_bf.astype(F32)
    d_hat = d_out * gain
    d_in = rstd * (d_hat - jnp.mean(d_hat, axis=-1, keepdims=True) - xhat * jnp.mean(d_hat * xhat, axis=-1, keepdims=True))
    d_v = (residual_bf.astype(F32) + d_in).astype(BF16)
    return d_v, jnp.sum(d_out * xhat, axis=0), jnp.sum(d_out, axis=0)


def gelu_pair(up):
    cdf = 0.5 * (1.0 + lax.erf(up * (0.5 ** 0.5)))
    slope = cdf + up * (jnp.exp(-0.5 * up * up) * ((2.0 * jnp.pi) ** -0.5))
    return (up * cdf).astype(BF16), slope


def layer_forward(h_in, params, length):
    w_att, w_up, w_down, vec, b_qkv, b_up = params
    n_qkv = b_qkv.shape[0]
    normed = layer_norm(h_in, vec[0], vec[1])
    qkv = (dot(normed, w_att[:n_qkv], NT) + b_qkv).astype(BF16)
    context = attn_fwd(qkv, length)
    mid = (h_in.astype(F32) + dot(context, w_att[n_qkv:], NN) + vec[2]).astype(BF16)
    normed2 = layer_norm(mid, vec[3], vec[4])
    up = dot(normed2, w_up, NT) + b_up
    hidden, slope = gelu_pair(up)
    out = (mid.astype(F32) + dot(hidden, w_down, NN) + vec[5]).astype(BF16)
    return out, (h_in, normed, qkv, context, mid, slope)


def layer_backward(g_out, saved, params, length):
    w_att, w_up, w_down, vec, b_qkv, _ = params
    n_qkv = b_qkv.shape[0]
    h_in, normed, qkv, context, mid, slope = saved
    d_hidden = dot(g_out, w_down, NT).astype(BF16)
    d_up = (d_hidden.astype(F32) * slope).astype(BF16)
    d_normed2 = dot(d_up, w_up, NN).astype(BF16)
    d_mid, d_gain2, d_bias2 = norm_back(mid, vec[3], d_normed2, g_out)
    d_context = dot(d_mid, w_att[n_qkv:], NT).astype(BF16)
    d_qkv = attn_bwd(qkv, d_context, length)
    d_normed = dot(d_qkv, w_att[:n_qkv], NN).astype(BF16)
    d_x, d_gain1, d_bias1 = norm_back(h_in, vec[0], d_normed, d_mid)
    d_b_attn = jnp.sum(d_mid, axis=0, dtype=F32)
    d_b_qkv = jnp.sum(d_qkv, axis=0, dtype=F32).reshape(3, -1)
    small = jnp.concatenate([jnp.stack([d_gain1, d_bias1, d_b_attn, d_gain2, d_bias2]), d_b_qkv])
    return d_x, (d_qkv, d_mid, context, normed, small)


def solution(mesh):
    n_dp, n_tp, n_pp = mesh.shape['dp'], mesh.shape['tp'], mesh.shape['pp']
    split = Mesh(mesh.devices.reshape(n_dp, n_tp, n_pp // 2, 2), ('dp', 'tp', 'py', 'core'))
    pp = ('py', 'core')
    act_spec = P('dp', None, None, None)
    param_specs = (P(pp, None), P(pp, None), P(pp, None, None, 'tp', None), P(pp, None, 'tp', None), P(pp, 'tp', None, None), P(pp, None), P(pp, None), P(pp, None), P(pp, None, 'tp'), P(pp, 'tp'), P(pp, 'tp', None), P(pp, None))
    gp = ('dp', 'py', 'core')
    grad_specs = (P(gp, None), P(gp, None), P(gp, None, None, 'tp', None), P(gp, None, 'tp', None), P(gp, 'tp', None, None), P(gp, None), P(gp, None), P(gp, None), P(gp, None, 'tp'), P(gp, 'tp'), P(gp, 'tp', None), P(gp, None))
    stage_spec = P(pp, 'dp', None, None, None)
    swap = [(0, 1), (1, 0)]

    def compute(x_in, seq_len, dy_out, *weights):
        (ln1_gain, ln1_bias, w_qkv, b_qkv, w_attn, b_attn, ln2_gain, ln2_bias, w_up, b_up, w_down, b_down) = tuple(weight[0] for weight in weights)
        dp_id, tp_id, py_id, core_id = (lax.axis_index(name) for name in ('dp', 'tp', 'py', 'core'))
        _, _, rows, width = x_in.shape
        n_local = w_attn.shape[0] * w_attn.shape[1]
        first_core, first_pair = core_id == 0, py_id == 0

        def by_core(on_first, on_second):
            return jnp.where(first_core, on_first, on_second)

        def gather_tp(value):
            return lax.all_gather(value, 'tp', axis=0)

        def core_swap(value):
            return lax.ppermute(value, 'core', swap)

        b_qkv_row = jnp.pad(b_qkv.reshape(1, -1), ((0, 0), (0, width - 3 * n_local)))
        packed = jnp.concatenate([jnp.stack([ln1_gain, ln1_bias, b_attn, ln2_gain, ln2_bias, b_down]), b_qkv_row, b_up.reshape(-1, width)])
        packed = gather_tp(packed)
        packed_other = core_swap(packed)
        packed = (by_core(packed, packed_other), by_core(packed_other, packed))

        att_shard = jnp.concatenate([w_qkv.reshape(3, width, n_local).transpose(0, 2, 1), w_attn.reshape(1, n_local, width)])
        shards = [att_shard, w_up.T.reshape(4, -1, width), w_down.reshape(4, -1, width)]
        pieces = ([], [])
        for shard in shards:
            mine = lax.dynamic_index_in_dim(shard, 2 * dp_id + core_id, 0, keepdims=False)
            theirs = lax.dynamic_index_in_dim(shard, 2 * dp_id + 1 - core_id, 0, keepdims=False)
            mine, theirs = with_layout_constraint(mine, ROW_MAJOR), with_layout_constraint(theirs, ROW_MAJOR)
            got = core_swap(theirs)
            pieces[0].append(by_core(mine, got))
            pieces[1].append(by_core(got, mine))

        gathered = [gather_tp(piece) for piece in pieces[0] + pieces[1]]
        from_x = []
        for own_x in gathered:
            from_x.append(lax.ppermute(own_x, 'dp', swap))

        def assemble(i):
            own_x, other_x = gathered[i], from_x[i]
            own_swapped = core_swap(own_x)
            full = jnp.zeros((4,) + own_x.shape, BF16)
            for row, x_pos, c_pos in ((own_swapped, dp_id, 1 - core_id), (own_x, dp_id, core_id), (other_x, 1 - dp_id, core_id), (core_swap(other_x), 1 - dp_id, 1 - core_id)):
                row, slot = lax.optimization_barrier((row, 2 * x_pos + c_pos))
                full = lax.dynamic_update_index_in_dim(full, row, slot, 0)
            return full.reshape(-1, width)

        def layer_params(layer):
            w_att, w_upt, w_dn = (assemble(i) for i in range(3 * layer, 3 * layer + 3))
            b_qkv_full = packed[layer][:, 6, :3 * n_local].reshape(n_tp, 3, n_local).transpose(1, 0, 2).reshape(-1)
            b_up_full = packed[layer][:, 7:].reshape(n_tp, 4, -1).transpose(1, 0, 2).reshape(-1)
            return (w_att, w_upt, w_dn, packed[layer][0, :6], b_qkv_full, b_up_full)

        params = (layer_params(0), layer_params(1))

        def my_sequence(array):
            return lax.dynamic_slice(array, (tp_id, core_id, 0, 0), (1, 1, rows, width)).reshape(rows, width)

        length = lax.dynamic_slice(seq_len, (tp_id, core_id), (1, 1)).reshape(1)

        def forward(h):
            mid, saved0 = layer_forward(h, params[0], length)
            out, saved1 = layer_forward(mid, params[1], length)
            return (mid, out), (saved0, saved1)

        def pair_pick(phase_a, phase_b):
            return jnp.where(first_pair, phase_a, phase_b)

        outs_a, saved_a = forward(my_sequence(x_in))
        outs_b, saved_b = forward(lax.ppermute(outs_a[1], 'py', [(0, 1)]))

        def own_stage(phase_a, phase_b):
            layers = [pair_pick(phase_a[layer], phase_b[layer]) for layer in range(2)]
            keep, other = by_core(*layers), core_swap(by_core(layers[1], layers[0]))
            return jnp.stack([by_core(keep, other), by_core(other, keep)])

        own_out = own_stage(outs_a, outs_b)
        own_mid = own_stage([saved[4] for saved in saved_a], [saved[4] for saved in saved_b])
        g_top, own_out, own_mid = lax.optimization_barrier((my_sequence(dy_out), own_out, own_mid))
        stage_out = gather_tp(own_out)
        mid_all = gather_tp(own_mid)

        def weight_payload(keep_a, keep_b):
            d_qkv_a, d_qkv_b = keep_a[0], keep_b[0]
            d_q, d_k, d_v = (pair_pick(d_qkv_a[:, i * width:(i + 1) * width], d_qkv_b[:, i * width:(i + 1) * width]) for i in range(3))
            d_mid, context, normed, small = (pair_pick(keep_a[i], keep_b[i]) for i in range(1, 5))
            got = core_swap(jnp.stack([by_core(d_v, d_q), by_core(context, d_k), normed, d_mid]))
            left0, left1 = by_core(d_q, d_v), by_core(d_k, context)
            right1 = by_core(normed, d_mid)
            grad0 = dot(left0, normed, TN) + dot(got[0], got[2], TN)
            grad1 = dot(left1, right1, TN) + dot(got[1], by_core(got[2], got[3]), TN)
            b_rows = small[5:].reshape(3, n_tp, n_local).transpose(1, 0, 2).reshape(n_tp, 1, 3 * n_local)
            b_rows = jnp.pad(b_rows, ((0, 0), (0, 2), (0, width - 3 * n_local)))
            return jnp.concatenate([grad0.reshape(n_tp, n_local, width), grad1.reshape(n_tp, n_local, width), jnp.broadcast_to(small[None, :5], (n_tp, 5, width)), b_rows], axis=1)

        def both_rows(gathered):
            other = core_swap(gathered)
            return jnp.stack([by_core(gathered, other), by_core(other, gathered)], axis=1)

        dx1_b, keep1_b = layer_backward(g_top, saved_b[1], params[1], length)
        dx0_b, keep0_b = layer_backward(dx1_b, saved_b[0], params[0], length)
        dx1_a, keep1_a = layer_backward(lax.ppermute(dx0_b, 'py', [(1, 0)]), saved_a[1], params[1], length)
        own_dx1, dx1_a, keep1_a = lax.optimization_barrier((pair_pick(dx1_a, dx1_b), dx1_a, keep1_a))
        dx1_all = both_rows(gather_tp(own_dx1))
        dx0_a, keep0_a = layer_backward(dx1_a, saved_a[0], params[0], length)
        own_dx0, payload1 = lax.optimization_barrier((pair_pick(dx0_a, dx0_b), weight_payload(keep1_a, keep1_b)))
        dx0_all = both_rows(gather_tp(own_dx0))
        reduced1 = lax.psum_scatter(payload1, 'tp', scatter_dimension=0, tiled=False)
        reduced0 = lax.psum_scatter(weight_payload(keep0_a, keep0_b), 'tp', scatter_dimension=0, tiled=False)

        stage_dx = by_core(dx0_all, dx1_all)
        from_next = lax.ppermute(dx0_all, pp, [(2, 1)])
        g_all = by_core(dx1_all, pair_pick(from_next, dy_out)).reshape(-1, width)

        reduced = by_core(reduced0, reduced1)
        reduced_other = core_swap(by_core(reduced1, reduced0))
        halves = by_core(reduced, reduced_other), by_core(reduced_other, reduced)
        g_qkv = jnp.concatenate([halves[0][:2 * n_local], halves[1][:n_local]]).reshape(3, n_local, width).transpose(0, 2, 1).reshape(w_qkv.shape)
        g_attn = halves[1][n_local:2 * n_local].reshape(w_attn.shape)
        g_vec = halves[0][2 * n_local:] + halves[1][2 * n_local:]

        normed2 = layer_norm(mid_all.reshape(-1, width), ln2_gain, ln2_bias)
        hidden, slope = gelu_pair(dot(normed2, w_up, NN) + b_up)
        d_up = dot(g_all, w_down, NT).astype(BF16).astype(F32) * slope
        g_w_up = dot(normed2, d_up.astype(BF16), TN)
        g_w_down = dot(hidden, g_all, TN)
        g_b_up = jnp.sum(d_up, axis=0)
        g_b_down = jnp.sum(g_all, axis=0, dtype=F32)

        grads = (g_vec[0], g_vec[1], g_qkv, g_vec[5, :3 * n_local].reshape(b_qkv.shape), g_attn, g_vec[2], g_vec[3], g_vec[4], g_w_up, g_b_up, g_w_down, g_b_down)
        return (stage_out[None], stage_dx[None]) + tuple(grad[None] for grad in grads)

    return jax.shard_map(compute, mesh=split, in_specs=(act_spec, P('dp', None), act_spec) + param_specs, out_specs=(stage_spec, stage_spec) + grad_specs, check_vma=False)
```

```python
import jax
import jax.numpy as jnp
from jax import lax
from jax.experimental import pallas as pl
from jax.experimental.pallas import tpu as pltpu
from jax.experimental.layout import Layout, with_layout_constraint
from jax.sharding import Mesh, PartitionSpec as P

LN_EPS = 1e-5
MASK_VALUE = -1e9
ROW_MAJOR = Layout((0, 1))
F32 = jnp.float32
BF16 = jnp.bfloat16
NT = (((1,), (1,)), ((), ()))
NN = (((1,), (0,)), ((), ()))
TN = (((0,), (0,)), ((), ()))


def dot(lhs, rhs, dims):
    return lax.dot_general(lhs, rhs, dims, preferred_element_type=F32)


def attn_fwd_kernel(len_ref, q_ref, k_ref, v_ref, ctx_ref):
    rows = q_ref.shape[0]
    key_ok = lax.broadcasted_iota(jnp.int32, (rows, rows), 1) < len_ref[0]
    parts = []
    for half in range(2):
        cols = slice(half * 64, half * 64 + 64)
        scores = dot(q_ref[:, cols], k_ref[:, cols], NT) * 0.125
        scores = jnp.where(key_ok, scores, MASK_VALUE)
        expd = jnp.exp(scores - jnp.max(scores, axis=-1, keepdims=True))
        prob = (expd * (1.0 / jnp.sum(expd, axis=-1, keepdims=True))).astype(BF16)
        parts.append(dot(prob, v_ref[:, cols], NN).astype(BF16))
    ctx_ref[...] = jnp.concatenate(parts, axis=1)


def attn_bwd_kernel(len_ref, q_ref, k_ref, v_ref, dctx_ref, dqkv_ref):
    rows = q_ref.shape[0]
    width = dqkv_ref.shape[1] // 3
    key_ok = lax.broadcasted_iota(jnp.int32, (rows, rows), 0) < len_ref[0]
    pieces = ([], [], [])
    for half in range(2):
        cols = slice(half * 64, half * 64 + 64)
        q, k, v, dctx = q_ref[:, cols], k_ref[:, cols], v_ref[:, cols], dctx_ref[:, cols]
        scores = dot(k, q, NT) * 0.125
        scores = jnp.where(key_ok, scores, MASK_VALUE)
        expd = jnp.exp(scores - jnp.max(scores, axis=0, keepdims=True))
        prob = expd * (1.0 / jnp.sum(expd, axis=0, keepdims=True))
        d_prob = dot(v, dctx, NT)
        delta = jnp.sum(d_prob * prob, axis=0, keepdims=True)
        d_scores = (prob * (d_prob - delta) * 0.125).astype(BF16)
        pieces[0].append(dot(d_scores, k, TN).astype(BF16))
        pieces[1].append(dot(d_scores, q, NN).astype(BF16))
        pieces[2].append(dot(prob.astype(BF16), dctx, NN).astype(BF16))
    pair = pl.program_id(0)
    for part in range(3):
        start = pl.multiple_of(part * width + pair * 128, 128)
        dqkv_ref[:, pl.ds(start, 128)] = jnp.concatenate(pieces[part], axis=1)


def col_spec(rows, offset):
    return pl.BlockSpec((rows, 128), lambda i: (0, offset + i))


SMEM_SPEC = pl.BlockSpec(memory_space=pltpu.SMEM)


def attn_fwd(qkv, length):
    rows, width = qkv.shape[0], qkv.shape[1] // 3
    pairs = width // 128
    return pl.pallas_call(
        attn_fwd_kernel,
        grid=(pairs,),
        out_shape=jax.ShapeDtypeStruct((rows, width), BF16),
        in_specs=[SMEM_SPEC] + [col_spec(rows, part * pairs) for part in range(3)],
        out_specs=col_spec(rows, 0),
        cost_estimate=pl.CostEstimate(flops=8 * pairs * rows * rows * 64 * 4, bytes_accessed=8 * rows * width, transcendentals=2 * pairs * rows * rows),
        name='attn_fwd',
    )(length, qkv, qkv, qkv)


def attn_bwd(qkv, dctx, length):
    rows, width = qkv.shape[0], qkv.shape[1] // 3
    pairs = width // 128
    return pl.pallas_call(
        attn_bwd_kernel,
        grid=(pairs,),
        out_shape=jax.ShapeDtypeStruct((rows, 3 * width), BF16),
        in_specs=[SMEM_SPEC] + [col_spec(rows, part * pairs) for part in range(3)] + [col_spec(rows, 0)],
        out_specs=pl.BlockSpec((rows, 3 * width), lambda i: (0, 0)),
        cost_estimate=pl.CostEstimate(flops=20 * pairs * rows * rows * 64 * 4, bytes_accessed=14 * rows * width, transcendentals=2 * pairs * rows * rows),
        name='attn_bwd',
    )(length, qkv, qkv, qkv, dctx)


def normalise(v_bf):
    v = v_bf.astype(F32)
    centred = v - jnp.mean(v, axis=-1, keepdims=True)
    rstd = lax.rsqrt(jnp.mean(centred * centred, axis=-1, keepdims=True) + LN_EPS)
    return centred * rstd, rstd


def layer_norm(v_bf, gain, bias):
    return (normalise(v_bf)[0] * gain + bias).astype(BF16)


def norm_back(v_bf, gain, d_out_bf, residual_bf):
    xhat, rstd = normalise(v_bf)
    d_out = d_out_bf.astype(F32)
    d_hat = d_out * gain
    d_in = rstd * (d_hat - jnp.mean(d_hat, axis=-1, keepdims=True) - xhat * jnp.mean(d_hat * xhat, axis=-1, keepdims=True))
    d_v = (residual_bf.astype(F32) + d_in).astype(BF16)
    return d_v, jnp.sum(d_out * xhat, axis=0), jnp.sum(d_out, axis=0)


def gelu_pair(up):
    cdf = 0.5 * (1.0 + lax.erf(up * (0.5 ** 0.5)))
    slope = cdf + up * (jnp.exp(-0.5 * up * up) * ((2.0 * jnp.pi) ** -0.5))
    return (up * cdf).astype(BF16), slope


def layer_forward(h_in, params, length):
    w_att, w_up, w_down, vec, b_qkv, b_up = params
    n_qkv = b_qkv.shape[0]
    normed = layer_norm(h_in, vec[0], vec[1])
    qkv = (dot(normed, w_att[:n_qkv], NT) + b_qkv).astype(BF16)
    context = attn_fwd(qkv, length)
    mid = (h_in.astype(F32) + dot(context, w_att[n_qkv:], NN) + vec[2]).astype(BF16)
    normed2 = layer_norm(mid, vec[3], vec[4])
    up = dot(normed2, w_up, NT) + b_up
    hidden, slope = gelu_pair(up)
    out = (mid.astype(F32) + dot(hidden, w_down, NN) + vec[5]).astype(BF16)
    return out, (h_in, normed, qkv, context, mid, slope)


def layer_backward(g_out, saved, params, length):
    w_att, w_up, w_down, vec, b_qkv, _ = params
    n_qkv = b_qkv.shape[0]
    h_in, normed, qkv, context, mid, slope = saved
    d_hidden = dot(g_out, w_down, NT).astype(BF16)
    d_up = (d_hidden.astype(F32) * slope).astype(BF16)
    d_normed2 = dot(d_up, w_up, NN).astype(BF16)
    d_mid, d_gain2, d_bias2 = norm_back(mid, vec[3], d_normed2, g_out)
    d_context = dot(d_mid, w_att[n_qkv:], NT).astype(BF16)
    d_qkv = attn_bwd(qkv, d_context, length)
    d_normed = dot(d_qkv, w_att[:n_qkv], NN).astype(BF16)
    d_x, d_gain1, d_bias1 = norm_back(h_in, vec[0], d_normed, d_mid)
    d_b_attn = jnp.sum(d_mid, axis=0, dtype=F32)
    d_b_qkv = jnp.sum(d_qkv, axis=0, dtype=F32).reshape(3, -1)
    small = jnp.concatenate([jnp.stack([d_gain1, d_bias1, d_b_attn, d_gain2, d_bias2]), d_b_qkv])
    return d_x, (d_qkv, d_mid, context, normed, small)


def solution(mesh):
    n_dp, n_tp, n_pp = mesh.shape['dp'], mesh.shape['tp'], mesh.shape['pp']
    split = Mesh(mesh.devices.reshape(n_dp, n_tp, n_pp // 2, 2), ('dp', 'tp', 'py', 'core'))
    pp = ('py', 'core')
    act_spec = P('dp', None, None, None)
    param_specs = (P(pp, None), P(pp, None), P(pp, None, None, 'tp', None), P(pp, None, 'tp', None), P(pp, 'tp', None, None), P(pp, None), P(pp, None), P(pp, None), P(pp, None, 'tp'), P(pp, 'tp'), P(pp, 'tp', None), P(pp, None))
    gp = ('dp', 'py', 'core')
    grad_specs = (P(gp, None), P(gp, None), P(gp, None, None, 'tp', None), P(gp, None, 'tp', None), P(gp, 'tp', None, None), P(gp, None), P(gp, None), P(gp, None), P(gp, None, 'tp'), P(gp, 'tp'), P(gp, 'tp', None), P(gp, None))
    stage_spec = P(pp, 'dp', None, None, None)
    swap = [(0, 1), (1, 0)]

    def compute(x_in, seq_len, dy_out, *weights):
        (ln1_gain, ln1_bias, w_qkv, b_qkv, w_attn, b_attn, ln2_gain, ln2_bias, w_up, b_up, w_down, b_down) = tuple(weight[0] for weight in weights)
        dp_id, tp_id, py_id, core_id = (lax.axis_index(name) for name in ('dp', 'tp', 'py', 'core'))
        _, _, rows, width = x_in.shape
        n_local = w_attn.shape[0] * w_attn.shape[1]
        first_core, first_pair = core_id == 0, py_id == 0

        def by_core(on_first, on_second):
            return jnp.where(first_core, on_first, on_second)

        def gather_tp(value):
            return lax.all_gather(value, 'tp', axis=0)

        def core_swap(value):
            return lax.ppermute(value, 'core', swap)

        b_qkv_row = jnp.pad(b_qkv.reshape(1, -1), ((0, 0), (0, width - 3 * n_local)))
        packed = jnp.concatenate([jnp.stack([ln1_gain, ln1_bias, b_attn, ln2_gain, ln2_bias, b_down]), b_qkv_row, b_up.reshape(-1, width)])
        packed = gather_tp(packed)
        packed_other = core_swap(packed)
        packed = (by_core(packed, packed_other), by_core(packed_other, packed))

        att_shard = jnp.concatenate([w_qkv.reshape(3, width, n_local).transpose(0, 2, 1), w_attn.reshape(1, n_local, width)])
        shards = [att_shard, w_up.T.reshape(4, -1, width), w_down.reshape(4, -1, width)]
        pieces = ([], [])
        for shard in shards:
            mine = lax.dynamic_index_in_dim(shard, 2 * dp_id + core_id, 0, keepdims=False)
            theirs = lax.dynamic_index_in_dim(shard, 2 * dp_id + 1 - core_id, 0, keepdims=False)
            mine, theirs = with_layout_constraint(mine, ROW_MAJOR), with_layout_constraint(theirs, ROW_MAJOR)
            got = core_swap(theirs)
            pieces[0].append(by_core(mine, got))
            pieces[1].append(by_core(got, mine))

        groups = (pieces[0][0][None], jnp.stack(pieces[0][1:]), jnp.stack(pieces[1]))
        gathered = []
        for group in groups:
            whole = gather_tp(group)
            gathered += [whole[:, j] for j in range(group.shape[0])]
        from_x = []
        for own_x in gathered:
            from_x.append(lax.ppermute(own_x, 'dp', swap))

        def assemble(i):
            own_x, other_x = gathered[i], from_x[i]
            own_swapped = core_swap(own_x)
            full = jnp.zeros((4,) + own_x.shape, BF16)
            for row, x_pos, c_pos in ((own_swapped, dp_id, 1 - core_id), (own_x, dp_id, core_id), (other_x, 1 - dp_id, core_id), (core_swap(other_x), 1 - dp_id, 1 - core_id)):
                row, slot = lax.optimization_barrier((row, 2 * x_pos + c_pos))
                full = lax.dynamic_update_index_in_dim(full, row, slot, 0)
            return full.reshape(-1, width)

        def layer_params(layer):
            w_att, w_upt, w_dn = (assemble(i) for i in range(3 * layer, 3 * layer + 3))
            b_qkv_full = packed[layer][:, 6, :3 * n_local].reshape(n_tp, 3, n_local).transpose(1, 0, 2).reshape(-1)
            b_up_full = packed[layer][:, 7:].reshape(n_tp, 4, -1).transpose(1, 0, 2).reshape(-1)
            return (w_att, w_upt, w_dn, packed[layer][0, :6], b_qkv_full, b_up_full)

        params = (layer_params(0), layer_params(1))

        def my_sequence(array):
            return lax.dynamic_slice(array, (tp_id, core_id, 0, 0), (1, 1, rows, width)).reshape(rows, width)

        length = lax.dynamic_slice(seq_len, (tp_id, core_id), (1, 1)).reshape(1)

        def forward(h):
            mid, saved0 = layer_forward(h, params[0], length)
            out, saved1 = layer_forward(mid, params[1], length)
            return (mid, out), (saved0, saved1)

        def pair_pick(phase_a, phase_b):
            return jnp.where(first_pair, phase_a, phase_b)

        def hop(value, source):
            return lax.ppermute(value, 'py', [(source, 1 - source)])

        outs_a, saved_a = forward(my_sequence(x_in))
        outs_b, saved_b = forward(hop(outs_a[1], 0))

        def split_gather(outs, saved, source):
            layers = [jnp.stack([outs[layer], saved[layer][4]]) for layer in range(2)]
            keep, other = by_core(*layers), core_swap(by_core(layers[1], layers[0]))
            row0, row1 = by_core(keep, other), by_core(other, keep)
            moved = hop(row1, source)
            near = gather_tp(jnp.where(py_id == source, row0, moved))
            return near, hop(near, 1 - source)

        near_a, far_a = split_gather(outs_a, saved_a, 0)
        near_b, far_b = split_gather(outs_b, saved_b, 1)
        row_sets = pair_pick(near_a, near_b), pair_pick(far_a, far_b)
        stage_out, mid_all = (jnp.stack([row_set[:, i] for row_set in row_sets], axis=1) for i in range(2))
        g_top = my_sequence(dy_out)

        def weight_payload(keep_a, keep_b):
            d_qkv_a, d_qkv_b = keep_a[0], keep_b[0]
            d_q, d_k, d_v = (pair_pick(d_qkv_a[:, i * width:(i + 1) * width], d_qkv_b[:, i * width:(i + 1) * width]) for i in range(3))
            d_mid, context, normed, small = (pair_pick(keep_a[i], keep_b[i]) for i in range(1, 5))
            got = core_swap(jnp.stack([by_core(d_v, d_q), by_core(context, d_k), normed, d_mid]))
            left0, left1 = by_core(d_q, d_v), by_core(d_k, context)
            right1 = by_core(normed, d_mid)
            grad0 = dot(left0, normed, TN) + dot(got[0], got[2], TN)
            grad1 = dot(left1, right1, TN) + dot(got[1], by_core(got[2], got[3]), TN)
            b_rows = small[5:].reshape(3, n_tp, n_local).transpose(1, 0, 2).reshape(n_tp, 1, 3 * n_local)
            b_rows = jnp.pad(b_rows, ((0, 0), (0, 2), (0, width - 3 * n_local)))
            return jnp.concatenate([grad0.reshape(n_tp, n_local, width), grad1.reshape(n_tp, n_local, width), jnp.broadcast_to(small[None, :5], (n_tp, 5, width)), b_rows], axis=1)

        def both_rows(gathered):
            other = core_swap(gathered)
            return jnp.stack([by_core(gathered, other), by_core(other, gathered)], axis=1)

        dx1_b, keep1_b = layer_backward(g_top, saved_b[1], params[1], length)
        dx0_b, keep0_b = layer_backward(dx1_b, saved_b[0], params[0], length)
        dx1_a, keep1_a = layer_backward(hop(dx0_b, 1), saved_a[1], params[1], length)
        own_dx1, dx1_a, keep1_a = lax.optimization_barrier((pair_pick(dx1_a, dx1_b), dx1_a, keep1_a))
        dx1_all = both_rows(gather_tp(own_dx1))
        dx0_a, keep0_a = layer_backward(dx1_a, saved_a[0], params[0], length)
        own_dx0, payload1 = lax.optimization_barrier((pair_pick(dx0_a, dx0_b), weight_payload(keep1_a, keep1_b)))
        dx0_all = both_rows(gather_tp(own_dx0))
        reduced1 = lax.psum_scatter(payload1, 'tp', scatter_dimension=0, tiled=False)
        payload0 = weight_payload(keep0_a, keep0_b)
        reduced0 = lax.psum_scatter(payload0, 'tp', scatter_dimension=0, tiled=False)

        stage_dx = by_core(dx0_all, dx1_all)
        from_next = lax.ppermute(dx0_all, pp, [(2, 1)])
        g_all = by_core(dx1_all, pair_pick(from_next, dy_out)).reshape(-1, width)

        reduced = by_core(reduced0, reduced1)
        reduced_other = core_swap(by_core(reduced1, reduced0))
        halves = by_core(reduced, reduced_other), by_core(reduced_other, reduced)
        g_qkv = jnp.concatenate([halves[0][:2 * n_local], halves[1][:n_local]]).reshape(3, n_local, width).transpose(0, 2, 1).reshape(w_qkv.shape)
        g_attn = halves[1][n_local:2 * n_local].reshape(w_attn.shape)
        g_vec = halves[0][2 * n_local:] + halves[1][2 * n_local:]

        normed2 = layer_norm(mid_all.reshape(-1, width), ln2_gain, ln2_bias)
        hidden, slope = gelu_pair(dot(normed2, w_up, NN) + b_up)
        d_up = dot(g_all, w_down, NT).astype(BF16).astype(F32) * slope
        g_w_up = dot(normed2, d_up.astype(BF16), TN)
        g_w_down = dot(hidden, g_all, TN)
        g_b_up = jnp.sum(d_up, axis=0)
        g_b_down = jnp.sum(g_all, axis=0, dtype=F32)

        grads = (g_vec[0], g_vec[1], g_qkv, g_vec[5, :3 * n_local].reshape(b_qkv.shape), g_attn, g_vec[2], g_vec[3], g_vec[4], g_w_up, g_b_up, g_w_down, g_b_down)
        return (stage_out[None], stage_dx[None]) + tuple(grad[None] for grad in grads)

    return jax.shard_map(compute, mesh=split, in_specs=(act_spec, P('dp', None), act_spec) + param_specs, out_specs=(stage_spec, stage_spec) + grad_specs, check_vma=False)
```

```python
import jax
import jax.numpy as jnp
from jax import lax
from jax.experimental import pallas as pl
from jax.experimental.pallas import tpu as pltpu
from jax.experimental.layout import Layout, with_layout_constraint
from jax.sharding import Mesh, PartitionSpec as P

LN_EPS = 1e-5
MASK_VALUE = -1e9
SCALE = 0.125
ROW_MAJOR = Layout((0, 1))
F32 = jnp.float32
BF16 = jnp.bfloat16
NT = (((1,), (1,)), ((), ()))
NN = (((1,), (0,)), ((), ()))
TN = (((0,), (0,)), ((), ()))


def dot(lhs, rhs, dims):
    return lax.dot_general(lhs, rhs, dims, preferred_element_type=F32)


def key_major_probs(q_scaled, k, key_ok):
    scores = jnp.where(key_ok, dot(k, q_scaled, NT), MASK_VALUE)
    expd = jnp.exp(scores - jnp.max(scores, axis=0, keepdims=True))
    return expd * (1.0 / jnp.sum(expd, axis=0, keepdims=True))


def attn_fwd_kernel(len_ref, q_ref, k_ref, v_ref, ctx_ref):
    rows = q_ref.shape[0]
    key_ok = lax.broadcasted_iota(jnp.int32, (rows, rows), 0) < len_ref[0]
    parts = []
    for half in range(2):
        cols = slice(half * 64, half * 64 + 64)
        prob = key_major_probs(q_ref[:, cols] * SCALE, k_ref[:, cols], key_ok)
        parts.append(dot(v_ref[:, cols], prob.astype(BF16), TN))
    ctx_ref[...] = jnp.concatenate(parts, axis=0).T.astype(BF16)


def attn_bwd_kernel(len_ref, q_ref, k_ref, v_ref, dctx_ref, dqkv_ref):
    rows = q_ref.shape[0]
    width = dqkv_ref.shape[1] // 3
    key_ok = lax.broadcasted_iota(jnp.int32, (rows, rows), 0) < len_ref[0]
    d_q, d_k, d_v = [], [], []
    for half in range(2):
        cols = slice(half * 64, half * 64 + 64)
        q, k, v, dctx = q_ref[:, cols] * SCALE, k_ref[:, cols], v_ref[:, cols], dctx_ref[:, cols]
        prob = key_major_probs(q, k, key_ok)
        d_prob = dot(v, dctx, NT)
        delta = jnp.sum(d_prob * prob, axis=0, keepdims=True)
        d_scores = (prob * (d_prob - delta)).astype(BF16)
        d_q.append(dot(k * SCALE, d_scores, TN))
        d_k.append(dot(d_scores, q, NN).astype(BF16))
        d_v.append(dot(prob.astype(BF16), dctx, NN).astype(BF16))
    pair = pl.program_id(0)
    whole = (jnp.concatenate(d_q, axis=0).T.astype(BF16), jnp.concatenate(d_k, axis=1), jnp.concatenate(d_v, axis=1))
    for part in range(3):
        start = pl.multiple_of(part * width + pair * 128, 128)
        dqkv_ref[:, pl.ds(start, 128)] = whole[part]


def col_spec(rows, offset):
    return pl.BlockSpec((rows, 128), lambda i: (0, offset + i))


SMEM_SPEC = pl.BlockSpec(memory_space=pltpu.SMEM)


def attn_fwd(qkv, length):
    rows, width = qkv.shape[0], qkv.shape[1] // 3
    pairs = width // 128
    return pl.pallas_call(
        attn_fwd_kernel,
        grid=(pairs,),
        out_shape=jax.ShapeDtypeStruct((rows, width), BF16),
        in_specs=[SMEM_SPEC] + [col_spec(rows, part * pairs) for part in range(3)],
        out_specs=col_spec(rows, 0),
        cost_estimate=pl.CostEstimate(flops=8 * pairs * rows * rows * 64 * 4, bytes_accessed=8 * rows * width, transcendentals=2 * pairs * rows * rows),
        name='attn_fwd',
    )(length, qkv, qkv, qkv)


def attn_bwd(qkv, dctx, length):
    rows, width = qkv.shape[0], qkv.shape[1] // 3
    pairs = width // 128
    return pl.pallas_call(
        attn_bwd_kernel,
        grid=(pairs,),
        out_shape=jax.ShapeDtypeStruct((rows, 3 * width), BF16),
        in_specs=[SMEM_SPEC] + [col_spec(rows, part * pairs) for part in range(3)] + [col_spec(rows, 0)],
        out_specs=pl.BlockSpec((rows, 3 * width), lambda i: (0, 0)),
        cost_estimate=pl.CostEstimate(flops=20 * pairs * rows * rows * 64 * 4, bytes_accessed=14 * rows * width, transcendentals=2 * pairs * rows * rows),
        name='attn_bwd',
    )(length, qkv, qkv, qkv, dctx)


def normalise(v_bf):
    v = v_bf.astype(F32)
    centred = v - jnp.mean(v, axis=-1, keepdims=True)
    rstd = lax.rsqrt(jnp.mean(centred * centred, axis=-1, keepdims=True) + LN_EPS)
    return centred * rstd, rstd


def layer_norm(v_bf, gain, bias):
    return (normalise(v_bf)[0] * gain + bias).astype(BF16)


def norm_back(v_bf, gain, d_out_bf, residual_bf):
    xhat, rstd = normalise(v_bf)
    d_out = d_out_bf.astype(F32)
    d_hat = d_out * gain
    d_in = rstd * (d_hat - jnp.mean(d_hat, axis=-1, keepdims=True) - xhat * jnp.mean(d_hat * xhat, axis=-1, keepdims=True))
    d_v = (residual_bf.astype(F32) + d_in).astype(BF16)
    return d_v, jnp.sum(d_out * xhat, axis=0), jnp.sum(d_out, axis=0)


def gelu_pair(up):
    cdf = 0.5 * (1.0 + lax.erf(up * (0.5 ** 0.5)))
    slope = cdf + up * (jnp.exp(-0.5 * up * up) * ((2.0 * jnp.pi) ** -0.5))
    return (up * cdf).astype(BF16), slope


def layer_forward(h_in, params, length):
    w_att, w_up, w_down, vec, b_qkv, b_up = params
    n_qkv = b_qkv.shape[0]
    normed = layer_norm(h_in, vec[0], vec[1])
    qkv = (dot(normed, w_att[:n_qkv], NT) + b_qkv).astype(BF16)
    context = attn_fwd(qkv, length)
    mid = (h_in.astype(F32) + dot(context, w_att[n_qkv:], NN) + vec[2]).astype(BF16)
    normed2 = layer_norm(mid, vec[3], vec[4])
    up = dot(normed2, w_up, NT) + b_up
    hidden, slope = gelu_pair(up)
    out = (mid.astype(F32) + dot(hidden, w_down, NN) + vec[5]).astype(BF16)
    return out, (h_in, normed, qkv, context, mid, slope)


def layer_backward(g_out, saved, params, length):
    w_att, w_up, w_down, vec, b_qkv, _ = params
    n_qkv = b_qkv.shape[0]
    h_in, normed, qkv, context, mid, slope = saved
    d_hidden = dot(g_out, w_down, NT).astype(BF16)
    d_up = (d_hidden.astype(F32) * slope).astype(BF16)
    d_normed2 = dot(d_up, w_up, NN).astype(BF16)
    d_mid, d_gain2, d_bias2 = norm_back(mid, vec[3], d_normed2, g_out)
    d_context = dot(d_mid, w_att[n_qkv:], NT).astype(BF16)
    d_qkv = attn_bwd(qkv, d_context, length)
    d_normed = dot(d_qkv, w_att[:n_qkv], NN).astype(BF16)
    d_x, d_gain1, d_bias1 = norm_back(h_in, vec[0], d_normed, d_mid)
    d_b_attn = jnp.sum(d_mid, axis=0, dtype=F32)
    d_b_qkv = jnp.sum(d_qkv, axis=0, dtype=F32).reshape(3, -1)
    small = jnp.concatenate([jnp.stack([d_gain1, d_bias1, d_b_attn, d_gain2, d_bias2]), d_b_qkv])
    return d_x, (d_qkv, d_mid, context, normed, small)


def solution(mesh):
    n_dp, n_tp, n_pp = mesh.shape['dp'], mesh.shape['tp'], mesh.shape['pp']
    split = Mesh(mesh.devices.reshape(n_dp, n_tp, n_pp // 2, 2), ('dp', 'tp', 'py', 'core'))
    pp = ('py', 'core')
    act_spec = P('dp', None, None, None)
    param_specs = (P(pp, None), P(pp, None), P(pp, None, None, 'tp', None), P(pp, None, 'tp', None), P(pp, 'tp', None, None), P(pp, None), P(pp, None), P(pp, None), P(pp, None, 'tp'), P(pp, 'tp'), P(pp, 'tp', None), P(pp, None))
    gp = ('dp', 'py', 'core')
    grad_specs = (P(gp, None), P(gp, None), P(gp, None, None, 'tp', None), P(gp, None, 'tp', None), P(gp, 'tp', None, None), P(gp, None), P(gp, None), P(gp, None), P(gp, None, 'tp'), P(gp, 'tp'), P(gp, 'tp', None), P(gp, None))
    stage_spec = P(pp, 'dp', None, None, None)
    swap = [(0, 1), (1, 0)]

    def compute(x_in, seq_len, dy_out, *weights):
        (ln1_gain, ln1_bias, w_qkv, b_qkv, w_attn, b_attn, ln2_gain, ln2_bias, w_up, b_up, w_down, b_down) = tuple(weight[0] for weight in weights)
        dp_id, tp_id, py_id, core_id = (lax.axis_index(name) for name in ('dp', 'tp', 'py', 'core'))
        _, _, rows, width = x_in.shape
        n_local = w_attn.shape[0] * w_attn.shape[1]
        first_core, first_pair = core_id == 0, py_id == 0

        def by_core(on_first, on_second):
            return jnp.where(first_core, on_first, on_second)

        def gather_tp(value):
            return lax.all_gather(value, 'tp', axis=0)

        def core_swap(value):
            return lax.ppermute(value, 'core', swap)

        b_qkv_row = jnp.pad(b_qkv.reshape(1, -1), ((0, 0), (0, width - 3 * n_local)))
        packed = jnp.concatenate([jnp.stack([ln1_gain, ln1_bias, b_attn, ln2_gain, ln2_bias, b_down]), b_qkv_row, b_up.reshape(-1, width)])
        packed = gather_tp(packed)
        packed_other = core_swap(packed)
        packed = (by_core(packed, packed_other), by_core(packed_other, packed))

        att_shard = jnp.concatenate([w_qkv.reshape(3, width, n_local).transpose(0, 2, 1), w_attn.reshape(1, n_local, width)])
        shards = [att_shard, w_up.T.reshape(4, -1, width), w_down.reshape(4, -1, width)]
        pieces = ([], [])
        for shard in shards:
            mine = lax.dynamic_index_in_dim(shard, 2 * dp_id + core_id, 0, keepdims=False)
            theirs = lax.dynamic_index_in_dim(shard, 2 * dp_id + 1 - core_id, 0, keepdims=False)
            mine, theirs = with_layout_constraint(mine, ROW_MAJOR), with_layout_constraint(theirs, ROW_MAJOR)
            got = core_swap(theirs)
            pieces[0].append(by_core(mine, got))
            pieces[1].append(by_core(got, mine))

        groups = (pieces[0][0][None], jnp.stack(pieces[0][1:]), jnp.stack(pieces[1]))
        gathered = []
        for group in groups:
            whole = gather_tp(group)
            gathered += [whole[:, j] for j in range(group.shape[0])]
        from_x = []
        for own_x in gathered:
            from_x.append(lax.ppermute(own_x, 'dp', swap))

        def assemble(i):
            own_x, other_x = gathered[i], from_x[i]
            own_swapped = core_swap(own_x)
            full = jnp.zeros((4,) + own_x.shape, BF16)
            for row, x_pos, c_pos in ((own_swapped, dp_id, 1 - core_id), (own_x, dp_id, core_id), (other_x, 1 - dp_id, core_id), (core_swap(other_x), 1 - dp_id, 1 - core_id)):
                row, slot = lax.optimization_barrier((row, 2 * x_pos + c_pos))
                full = lax.dynamic_update_index_in_dim(full, row, slot, 0)
            return full.reshape(-1, width)

        def layer_params(layer):
            w_att, w_upt, w_dn = (assemble(i) for i in range(3 * layer, 3 * layer + 3))
            b_qkv_full = packed[layer][:, 6, :3 * n_local].reshape(n_tp, 3, n_local).transpose(1, 0, 2).reshape(-1)
            b_up_full = packed[layer][:, 7:].reshape(n_tp, 4, -1).transpose(1, 0, 2).reshape(-1)
            return (w_att, w_upt, w_dn, packed[layer][0, :6], b_qkv_full, b_up_full)

        params = (layer_params(0), layer_params(1))

        def my_sequence(array):
            return lax.dynamic_slice(array, (tp_id, core_id, 0, 0), (1, 1, rows, width)).reshape(rows, width)

        length = lax.dynamic_slice(seq_len, (tp_id, core_id), (1, 1)).reshape(1)

        def forward(h):
            mid, saved0 = layer_forward(h, params[0], length)
            out, saved1 = layer_forward(mid, params[1], length)
            return (mid, out), (saved0, saved1)

        def pair_pick(phase_a, phase_b):
            return jnp.where(first_pair, phase_a, phase_b)

        def hop(value, source):
            return lax.ppermute(value, 'py', [(source, 1 - source)])

        outs_a, saved_a = forward(my_sequence(x_in))
        outs_b, saved_b = forward(hop(outs_a[1], 0))

        def split_gather(out, mid, source):
            moved, out, pair_id = lax.optimization_barrier((hop(mid, source), out, py_id))
            near = gather_tp(jnp.where(pair_id == source, out, moved))
            return near, hop(near, 1 - source)

        def own_rows(layer0, layer1):
            keep, other = by_core(layer0, layer1), core_swap(by_core(layer1, layer0))
            return jnp.stack([by_core(keep, other), by_core(other, keep)], axis=1)

        moves_a = [split_gather(outs_a[layer], saved_a[layer][4], 0) for layer in range(2)]
        moves_b = [split_gather(outs_b[layer], saved_b[layer][4], 1) for layer in range(2)]
        stage_out, mid_all = (own_rows(*(pair_pick(moves_a[layer][i], moves_b[layer][i]) for layer in range(2))) for i in range(2))
        g_top = my_sequence(dy_out)

        def weight_payload(keep_a, keep_b):
            d_qkv_a, d_qkv_b = keep_a[0], keep_b[0]
            d_q, d_k, d_v = (pair_pick(d_qkv_a[:, i * width:(i + 1) * width], d_qkv_b[:, i * width:(i + 1) * width]) for i in range(3))
            d_mid, context, normed, small = (pair_pick(keep_a[i], keep_b[i]) for i in range(1, 5))
            got = core_swap(jnp.stack([by_core(d_v, d_q), by_core(context, d_k), normed, d_mid]))
            left0, left1 = by_core(d_q, d_v), by_core(d_k, context)
            right1 = by_core(normed, d_mid)
            grad0 = dot(left0, normed, TN) + dot(got[0], got[2], TN)
            grad1 = dot(left1, right1, TN) + dot(got[1], by_core(got[2], got[3]), TN)
            b_rows = small[5:].reshape(3, n_tp, n_local).transpose(1, 0, 2).reshape(n_tp, 1, 3 * n_local)
            b_rows = jnp.pad(b_rows, ((0, 0), (0, 2), (0, width - 3 * n_local)))
            return jnp.concatenate([grad0.reshape(n_tp, n_local, width), grad1.reshape(n_tp, n_local, width), jnp.broadcast_to(small[None, :5], (n_tp, 5, width)), b_rows], axis=1)

        def both_rows(gathered):
            other = core_swap(gathered)
            return jnp.stack([by_core(gathered, other), by_core(other, gathered)], axis=1)

        dx1_b, keep1_b = layer_backward(g_top, saved_b[1], params[1], length)
        dx0_b, keep0_b = layer_backward(dx1_b, saved_b[0], params[0], length)
        dx1_a, keep1_a = layer_backward(hop(dx0_b, 1), saved_a[1], params[1], length)
        own_dx1, dx1_a, keep1_a = lax.optimization_barrier((pair_pick(dx1_a, dx1_b), dx1_a, keep1_a))
        dx1_all = both_rows(gather_tp(own_dx1))
        dx0_a, keep0_a = layer_backward(dx1_a, saved_a[0], params[0], length)
        own_dx0, payload1 = lax.optimization_barrier((pair_pick(dx0_a, dx0_b), weight_payload(keep1_a, keep1_b)))
        dx0_all = both_rows(gather_tp(own_dx0))
        payload = jnp.concatenate([weight_payload(keep0_a, keep0_b), payload1], axis=1)
        both_reduced = lax.psum_scatter(payload, 'tp', scatter_dimension=0, tiled=False)
        reduced0, reduced1 = jnp.split(both_reduced, 2)

        stage_dx = by_core(dx0_all, dx1_all)
        from_next = lax.ppermute(dx0_all, pp, [(2, 1)])
        g_all = by_core(dx1_all, pair_pick(from_next, dy_out)).reshape(-1, width)

        reduced = by_core(reduced0, reduced1)
        reduced_other = core_swap(by_core(reduced1, reduced0))
        halves = by_core(reduced, reduced_other), by_core(reduced_other, reduced)
        g_qkv = jnp.concatenate([halves[0][:2 * n_local], halves[1][:n_local]]).reshape(3, n_local, width).transpose(0, 2, 1).reshape(w_qkv.shape)
        g_attn = halves[1][n_local:2 * n_local].reshape(w_attn.shape)
        g_vec = halves[0][2 * n_local:] + halves[1][2 * n_local:]

        normed2 = layer_norm(mid_all.reshape(-1, width), ln2_gain, ln2_bias)
        hidden, slope = gelu_pair(dot(normed2, w_up, NN) + b_up)
        d_up = dot(g_all, w_down, NT).astype(BF16).astype(F32) * slope
        g_w_up = dot(normed2, d_up.astype(BF16), TN)
        g_w_down = dot(hidden, g_all, TN)
        g_b_up = jnp.sum(d_up, axis=0)
        g_b_down = jnp.sum(g_all, axis=0, dtype=F32)

        grads = (g_vec[0], g_vec[1], g_qkv, g_vec[5, :3 * n_local].reshape(b_qkv.shape), g_attn, g_vec[2], g_vec[3], g_vec[4], g_w_up, g_b_up, g_w_down, g_b_down)
        return (stage_out[None], stage_dx[None]) + tuple(grad[None] for grad in grads)

    return jax.shard_map(compute, mesh=split, in_specs=(act_spec, P('dp', None), act_spec) + param_specs, out_specs=(stage_spec, stage_spec) + grad_specs, check_vma=False)
```
